32 devices in a mesh: rep: 2 (over z, core), dp: 16 (over x, y).
Axes of the slice: x: 4, y: 4, z: 1, core: 2. Of those that a mesh axis runs over, the one named last changes fastest.
The devices are a block of a 4x4x8 slice.
Arguments:
- x: bfloat16 [32, 4096, 512], P(('rep', 'dp')), parts along dimension 0
- dy: bfloat16 [32, 4096, 512], P(('rep', 'dp')), parts along dimension 0
- w_gate: bfloat16 [2, 512, 2048], P(None, 'dp')
- w_up: bfloat16 [2, 512, 2048], P(None, 'dp')
- w_down: bfloat16 [2, 2048, 512], P(None, 'dp')
Outputs:
- output 1: bfloat16 [32, 4096, 512], P(('rep', 'dp')), parts along dimension 0
- output 2: bfloat16 [4, 512, 2048], P('rep', 'dp'), parts along dimension 0
- output 3: bfloat16 [4, 512, 2048], P('rep', 'dp'), parts along dimension 0
- output 4: bfloat16 [4, 2048, 512], P('rep', 'dp'), parts along dimension 0
There are 2 independent parts. The reference program is written for one: setup_inputs(seed, part) draws one part's arguments, and reference() takes and returns one part's arrays. A program takes and returns all parts, laid end to end along the dimension named above; an argument that names none is the same for every part.
All inputs are finite; a program needn't handle non-finite values.
Results may differ from the reference program's by a relative error of at most 0.018.
Values are sent between devices in bfloat16 or wider.
A program may use at most 768 MiB of HBM per device.

```python
import jax
import jax.numpy as jnp
from jax import lax

SEQUENCES = 16
TOKENS = 4096
D = 512
FF = 2048
LAYERS = 2
NAMES = ("w_gate", "w_up", "w_down")
SHAPES = {"w_gate": (LAYERS, D, FF), "w_up": (LAYERS, D, FF), "w_down": (LAYERS, FF, D)}


def bump(key, n, height):
    away = (jnp.arange(n, dtype=jnp.int32) - jax.random.randint(key, (), 0, n, jnp.int32)) % n
    return jnp.where(away < n // 8, height, 1.0)


def together(key, own, strength):
    shared = jax.random.normal(key, own.shape[1:], jnp.float32)
    return (own + strength * shared) * lax.rsqrt(1 + strength * strength)


def setup_inputs(seed: int = 0, part: int = 0) -> dict:
    kx, kdy, ka, kb, kz, kf, kh, kl, *kw = jax.random.split(jax.random.key(seed), 8 + len(NAMES))
    kx, kdy, ka, kb = (jax.random.fold_in(k, part) for k in (kx, kdy, ka, kb))
    shape = (SEQUENCES, TOKENS, D)
    much_x, much_dy = jax.random.uniform(kz, (2,), jnp.float32, 0.0, 1.0)
    layers = 2.0 ** jax.random.uniform(kl, (LAYERS, 1, 1), jnp.float32, -1.0, 1.0)
    x = together(ka, jax.random.normal(kx, shape, jnp.float32), much_x) * bump(kf, D, 4.0)
    dy = together(kb, jax.random.normal(kdy, shape, jnp.float32), much_dy)
    drawn = {"x": x.astype(jnp.bfloat16), "dy": (dy * (SEQUENCES * TOKENS) ** -0.5).astype(jnp.bfloat16)}
    for key, name in zip(kw, NAMES, strict=True):
        w = jax.random.normal(key, SHAPES[name], jnp.float32) * SHAPES[name][1] ** -0.5
        drawn[name] = (w * {"w_gate": 1.0, "w_up": bump(kh, FF, 4.0), "w_down": layers}[name]).astype(jnp.bfloat16)
    return drawn


def matmul(a, w):
    return jnp.dot(a, w, preferred_element_type=jnp.float32).astype(jnp.bfloat16)


def normed(h):
    wide = h.astype(jnp.float32)
    scale = lax.rsqrt(jnp.mean(wide**2, -1, keepdims=True) + 1e-6)
    return (wide * scale).astype(jnp.bfloat16)


def layer(h, w):
    a = normed(h)
    gate = jnp.dot(a, w["w_gate"], preferred_element_type=jnp.float32)
    up = jnp.dot(a, w["w_up"], preferred_element_type=jnp.float32)
    return h + matmul((jax.nn.silu(gate) * up).astype(jnp.bfloat16), w["w_down"])


def stack(weights, h):
    return lax.scan(lambda h, w: (layer(h, w), None), h, weights)[0]


def reference(x, dy, w_gate, w_up, w_down):
    weights = dict(zip(NAMES, (w_gate, w_up, w_down), strict=True))

    def take(so_far, sequence):
        h, by_y = sequence
        _, back = jax.vjp(stack, weights, h)
        by_weights, by_h = back(by_y)
        return jax.tree.map(lambda total, term: total + term.astype(jnp.float32), so_far, by_weights), by_h

    none_yet = {name: jnp.zeros(w.shape, jnp.float32) for name, w in weights.items()}
    by_weights, by_x = lax.scan(take, none_yet, (x, dy))
    return (by_x, *(by_weights[name].astype(jnp.bfloat16) for name in NAMES))
```

```python
import functools
import math

import jax
import jax.numpy as jnp
from jax import lax
from jax.experimental import pallas as pl
from jax.experimental.pallas import tpu as pltpu
from jax.sharding import PartitionSpec as P

F32, BF16 = jnp.float32, jnp.bfloat16
CHUNKS = 4
TILES = 8
EPS = 1e-6
HALVES = 2


def dot(a, b, ca, cb):
    return lax.dot_general(a, b, (((ca,), (cb,)), ((), ())), preferred_element_type=F32)


def kernel(
    side, layers, x_hbm, dy_hbm, gate_own, up_own, down_hbm, dx_hbm, out_gate, out_up, out_down, kept_hbm,
    w, h, a, dh, acc, g, s_tile, kept, order, fin, st1, st2, st3, st4, rc1, rc2, rc3, rc4,
    load_sem, keep_sem, ag_send, ag_recv, rs_send, rs_recv,
):
    tokens, d = h.shape[1:]
    rows, hid = w.shape[4:]
    tile = tokens // TILES
    half, quarter = hid // 2, hid // 4
    units = layers * CHUNKS
    me = lax.axis_index("dp")
    px, py = me // side, me % side
    xs = {k: (px + k + side) % side for k in (-1, 0, 1, 2)}
    ys = {k: (py + k + side) % side for k in (-1, 0, 1, 2)}
    beside = {
        ("x", 1): xs[1] * side + py,
        ("x", -1): xs[-1] * side + py,
        ("y", 1): px * side + ys[1],
        ("y", -1): px * side + ys[-1],
    }

    load_x = pltpu.make_async_copy(x_hbm, h.at[0], load_sem.at[0])
    load_dy = pltpu.make_async_copy(dy_hbm, dh, load_sem.at[1])
    load_w = pltpu.make_async_copy(down_hbm, w.at[:, 2, px, py], load_sem.at[2])
    load_w.start()
    load_x.start()
    load_dy.start()

    many = hid // (CHUNKS * rows)
    source = lax.broadcasted_iota(jnp.int32, (hid, hid), 0)
    goal = lax.broadcasted_iota(jnp.int32, (hid, hid), 1)
    chunk_of, place = goal // (many * rows), goal % (many * rows)
    at_source = (place // rows) * (CHUNKS * rows) + chunk_of * rows + place % rows
    order[...] = jnp.where(source == at_source, 1.0, 0.0).astype(BF16)
    run = many * rows
    owns = [(l, k, ref) for l in range(layers) for k, ref in enumerate((gate_own, up_own))]
    for q in range(CHUNKS):
        both = jnp.concatenate([ref[l, :, pl.ds(q * hid, hid)] for l, _, ref in owns], 0)
        moved = dot(both, order[...], 1, 0).astype(BF16)
        for n, (l, k, _) in enumerate(owns):
            for j in range(CHUNKS):
                piece = moved[n * rows : (n + 1) * rows, j * run : (j + 1) * run]
                w[l * CHUNKS + j, k, px, py, :, pl.ds(q * run, run)] = piece

    def finish(l):
        for q in range(CHUNKS):
            both = jnp.concatenate(
                [
                    jnp.concatenate([fin[j, k, :, pl.ds(q * run, run)] for j in range(CHUNKS)], 1)
                    for k in range(2)
                ],
                0,
            )
            moved = dot(both, order[...], 1, 1).astype(BF16)
            for k, ref in enumerate((out_gate, out_up)):
                ref[l, :, pl.ds(q * hid, hid)] = moved[k * rows : (k + 1) * rows]

    barrier = pltpu.get_barrier_semaphore()
    for target in beside.values():
        pl.semaphore_signal(barrier, inc=1, device_id={"dp": target})
    pl.semaphore_wait(barrier, len(beside))

    def gather_copies(u, s):
        copies = []
        for colour in range(2):
            axis = ("x", "y")[(colour + (s > 2)) % 2]
            for way, sign in ((0, 1), (1, -1)):
                lo = colour * half
                if s % 2:
                    lanes, at = pl.ds(lo, half), 0
                else:
                    lanes, at = pl.ds(lo + way * quarter, quarter), -sign
                pos = (xs if axis == "x" else ys)[at]
                if s <= 2:
                    i, j = (pos, py) if axis == "x" else (px, pos)
                else:
                    i, j = (pos, slice(None)) if axis == "x" else (slice(None), pos)
                ref = w.at[u, :, i, j, :, lanes]
                k = colour * 2 + way
                copies.append(
                    pltpu.make_async_remote_copy(
                        src_ref=ref,
                        dst_ref=ref,
                        send_sem=ag_send.at[u, s - 1, k],
                        recv_sem=ag_recv.at[u, s - 1, k],
                        device_id={"dp": beside[axis, sign]},
                    )
                )
        return copies

    def gather_tick(k):
        for s in (5, 4, 3, 2, 1):
            u = k - s + 1

            def step(s=s, u=u):
                if s > 1:
                    for copy in gather_copies(u, s - 1):
                        copy.wait()
                if s < 5:
                    for copy in gather_copies(u, s):
                        copy.start()

            if isinstance(u, int):
                if 0 <= u < units:
                    step()
            else:
                pl.when(jnp.logical_and(u >= 0, u < units))(step)

    def reduce_copies(s):
        st, rc = ((st1, rc1), (st2, rc2), (st3, rc3), (st4, rc4))[s - 1]
        copies = []
        for colour in range(2):
            axis = ("x", "y")[(colour + (s > 2)) % 2]
            for way, sign in ((0, 1), (1, -1)):
                copies.append(
                    pltpu.make_async_remote_copy(
                        src_ref=st.at[colour, way],
                        dst_ref=rc.at[colour, way],
                        send_sem=rs_send.at[s - 1, colour * 2 + way],
                        recv_sem=rs_recv.at[s - 1, colour * 2 + way],
                        device_id={"dp": beside[axis, sign]},
                    )
                )
        return copies

    def part(par, colour, s, k, lo, n):
        axis = ("x", "y")[(colour + (s > 2)) % 2]
        pos = (xs if axis == "x" else ys)[k]
        lanes = pl.ds(colour * half + lo, n)
        if s <= 2:
            i, j = (pos, slice(None)) if axis == "x" else (slice(None), pos)
        else:
            i, j = (pos, py) if axis == "x" else (px, pos)
        return g.at[par, :, i, j, :, lanes]

    def begin(par, s):
        for colour in range(2):
            for way in range(2):
                (st1 if s == 1 else st3)[colour, way] = part(par, colour, s, 2, way * quarter, quarter)[...].astype(BF16)
        for copy in reduce_copies(s):
            copy.start()

    def middle(par, s):
        for copy in reduce_copies(s - 1):
            copy.wait()
        st, rc = (st2, rc1) if s == 2 else (st4, rc3)
        for colour in range(2):
            for way, sign in ((0, 1), (1, -1)):
                took, kept = way * quarter, (1 - way) * quarter
                st[colour, way, ..., pl.ds(took, quarter)] = (
                    part(par, colour, s, sign, took, quarter)[...] + rc[colour, way].astype(F32)
                ).astype(BF16)
                st[colour, way, ..., pl.ds(kept, quarter)] = part(par, colour, s, sign, kept, quarter)[...].astype(BF16)
        for copy in reduce_copies(s):
            copy.start()

    def reduce_tick(n, par, u):
        if n == 1:
            begin(par, 1)
        elif n == 2:
            middle(par, 2)
        elif n == 3:
            for copy in reduce_copies(2):
                copy.wait()
            for colour in range(2):
                own = part(par, colour, 2, 0, 0, half)
                own[...] = own[...] + rc2[colour, 0].astype(F32) + rc2[colour, 1].astype(F32)
            begin(par, 3)
        elif n == 4:
            middle(par, 4)
        else:
            for copy in reduce_copies(4):
                copy.wait()
            for colour in range(2):
                own = part(par, colour, 4, 0, 0, half)[...]
                total = own + rc4[colour, 0].astype(F32) + rc4[colour, 1].astype(F32)
                lanes = pl.ds(colour * half, half)
                fin[u % CHUNKS, :, :, lanes] = total[:2].astype(BF16)
                out_down[u, :, lanes] = total[2].astype(BF16)

    def at(t):
        return pl.ds(pl.multiple_of(t * tile, tile), tile)

    def matrix(u, k):
        return w[u, k].reshape(d, hid)

    def norm(l, t):
        wide = h[l, at(t)].astype(F32)
        scale = lax.rsqrt(jnp.mean(wide * wide, -1, keepdims=True) + EPS)
        a[l, at(t)] = (wide * scale).astype(BF16)

    def loop(n, body):
        lax.fori_loop(0, n, lambda i, c: (body(i), c)[1], 0)

    def keep(i):
        return pltpu.make_async_copy(kept.at[i % 2], kept_hbm.at[i], keep_sem.at[i % 2])

    def fetch(i):
        return pltpu.make_async_copy(kept_hbm.at[i], kept.at[i % 2], keep_sem.at[i % 2])

    def fwd1(i):
        u, t = i // TILES, i % TILES
        rowsa = a[0, at(t)]
        gate = dot(rowsa, matrix(u, 0), 1, 0)
        up = dot(rowsa, matrix(u, 1), 1, 0)
        kept[i % 2, 0] = gate
        kept[i % 2, 1] = up
        s_tile[i % 2, 2] = (gate * jax.nn.sigmoid(gate) * up).astype(BF16)

    def fwd2(i):
        u, t = i // TILES, i % TILES
        new = dot(s_tile[i % 2, 2], matrix(u, 2), 1, 0)
        acc[at(t)] = jnp.where(u == 0, 0.0, acc[at(t)]) + new

    def fwd_end(t):
        first = h[0, at(t)].astype(F32) + acc[at(t)].astype(BF16).astype(F32)
        h[1, at(t)] = first.astype(BF16)
        norm(1, t)

    def bwd1(l, i, late=False):
        u, t = l * CHUNKS + i // TILES, i % TILES
        n = tile // HALVES
        for r in range(HALVES):
            q = pl.ds(r * n, n)
            rr = pl.ds(pl.multiple_of(t * tile + r * n, n), n)
            if l:
                rowsa = a[l, rr]
                gate = dot(rowsa, matrix(u, 0), 1, 0)
                up = dot(rowsa, matrix(u, 1), 1, 0)
            else:
                gate, up = kept[i % 2, 0, q], kept[i % 2, 1, q]
            by = dot(dh[rr], matrix(u, 2), 1, 1).astype(BF16).astype(F32)
            sig = jax.nn.sigmoid(gate)
            silu = gate * sig
            by_gate = (by * up * (sig + silu * (1.0 - sig))).astype(BF16)
            by_up = (by * silu).astype(BF16)
            if late:
                h[1, rr] = by_gate
                a[1, rr] = by_up
            else:
                s_tile[i % 2, 0, q] = by_gate
                s_tile[i % 2, 1, q] = by_up
            s_tile[i % 2, 2, q] = (silu * up).astype(BF16)

    def by_hidden(i, late):
        t = i % TILES
        return (h[1, at(t)], a[1, at(t)]) if late else (s_tile[i % 2, 0], s_tile[i % 2, 1])

    def bwd_in(l, i, late=False):
        chunk, t = i // TILES, i % TILES
        u = l * CHUNKS + chunk
        by_gate, by_up = by_hidden(i, late)
        new = dot(by_gate, matrix(u, 0), 1, 1) + dot(by_up, matrix(u, 1), 1, 1)
        acc[at(t)] = jnp.where(chunk == 0, 0.0, acc[at(t)]) + new

    def bwd_w(l, i, late=False):
        chunk, t = i // TILES, i % TILES
        par = chunk % 2
        by_gate, by_up = by_hidden(i, late)
        rowsa = a[l, at(t)]
        for k, (p, q) in enumerate(((rowsa, by_gate), (rowsa, by_up), (s_tile[i % 2, 2], dh[at(t)]))):
            old = jnp.where(t == 0, 0.0, g[par, k])
            g[par, k] = old + dot(p, q, 0, 0).reshape(old.shape)

    def bwd_end(l, t):
        wide = h[l, at(t)].astype(F32)
        scale = lax.rsqrt(jnp.mean(wide * wide, -1, keepdims=True) + EPS)
        da = acc[at(t)].astype(BF16).astype(F32)
        along = jnp.mean(da * wide, -1, keepdims=True)
        by = (da * scale - wide * (scale * scale * scale * along)).astype(BF16)
        dh[at(t)] = (dh[at(t)].astype(F32) + by.astype(F32)).astype(BF16)

    load_w.wait()
    gather_tick(0)
    gather_tick(1)
    load_x.wait()
    loop(TILES // 2, lambda t: norm(0, t))
    gather_tick(2)
    loop(TILES - TILES // 2, lambda t: norm(0, t + TILES // 2))
    gather_tick(3)
    gather_tick(4)

    steps = CHUNKS * TILES
    fwd1(0)
    keep(0).start()

    def fwd_step(i):
        @pl.when(i % TILES == 0)
        def _():
            gather_tick(4 + i // TILES)

        @pl.when(i >= 2)
        def _():
            keep(i - 2).wait()

        fwd1(i)
        fwd2(i - 1)
        keep(i).start()

    loop(steps - 1, lambda i: fwd_step(i + 1))
    fwd2(steps - 1)
    loop(TILES, fwd_end)
    load_dy.wait()
    gather_tick(4 + CHUNKS)
    for i in (steps - 2, steps - 1):
        keep(i).wait()
    for i in range(2):
        fetch(i).start()

    when = ((1, 1), (2, 3), (3, 5), (4, 6), (5, 7))

    def step1(i):
        chunk, t = i // TILES, i % TILES

        @pl.when(t == 0)
        def _():
            gather_tick(4 + CHUNKS + chunk)

        for tick, place in when:

            @pl.when(jnp.logical_and(t == place, chunk > 0))
            def _(tick=tick):
                reduce_tick(tick, (chunk + 1) % 2, CHUNKS + chunk - 1)

        bwd_w(1, i - 1)
        bwd_in(1, i - 1)
        bwd1(1, i)

    bwd1(1, 0)
    loop(steps - 1, lambda i: step1(i + 1))
    bwd_in(1, steps - 1)
    bwd_w(1, steps - 1)
    loop(TILES, lambda t: bwd_end(1, t))

    def ticks(chunk, t):
        for tick, place in when:

            @pl.when(t == place)
            def _(tick=tick):
                reduce_tick(tick, (chunk + 1) % 2, (chunk + 2 * CHUNKS - 1) % (2 * CHUNKS))
                if tick == 5:
                    pl.when(chunk == 0)(lambda: finish(1))

    def step0(i):
        ticks(i // TILES, i % TILES)
        fetch(i + 1).start()
        fetch(i).wait()
        bwd_w(0, i - 1)
        bwd_in(0, i - 1)
        bwd1(0, i)

    def step0_late(i):
        ticks(i // TILES, i % TILES)
        pl.when(i + 1 < steps)(lambda: fetch(i + 1).start())
        fetch(i).wait()
        bwd1(0, i, True)
        bwd_w(0, i - 1, True)

    fetch(0).wait()
    bwd1(0, 0)
    early = steps - TILES
    loop(early - 1, lambda i: step0(i + 1))
    fetch(early + 1).start()
    fetch(early).wait()
    bwd1(0, early, True)
    bwd_in(0, early - 1)
    bwd_w(0, early - 1)
    loop(TILES - 1, lambda i: step0_late(i + early + 1))
    bwd_w(0, steps - 1, True)

    def end0(t):
        bwd_in(0, early + t, True)
        bwd_end(0, t)

    done = 0
    for tick, share in ((1, 2), (2, 3), (3, 1), (4, 2), (5, 0)):
        reduce_tick(tick, (CHUNKS - 1) % 2, CHUNKS - 1)
        if share:
            loop(share, lambda t, done=done: end0(t + done))
        done += share
        if tick == 4:
            store = pltpu.make_async_copy(dh, dx_hbm, load_sem.at[0])
            store.start()
    finish(0)
    store.wait()


def solution(mesh):
    ways = mesh.shape["dp"]
    side = math.isqrt(ways)

    def step(x, dy, w_gate, w_up, w_down):
        layers, rows, ff = w_gate.shape
        tokens, d = x.shape[1:]
        hid = ff // CHUNKS
        own = w_down.shape[1] // CHUNKS
        assert rows == own and d == hid and layers == 2
        units = layers * CHUNKS

        hbm, vmem = (pl.BlockSpec(memory_space=m) for m in (pl.ANY, pltpu.VMEM))
        tile = tokens // TILES
        quarter, half = hid // 4, hid // 2
        by_x, by_gate, by_up, by_down, _ = pl.pallas_call(
            functools.partial(kernel, side, layers),
            out_shape=(
                jax.ShapeDtypeStruct((tokens, d), BF16),
                jax.ShapeDtypeStruct(w_gate.shape, BF16),
                jax.ShapeDtypeStruct(w_up.shape, BF16),
                jax.ShapeDtypeStruct((units, rows, hid), BF16),
                jax.ShapeDtypeStruct((CHUNKS * TILES, 2, tile, hid), F32),
            ),
            in_specs=[hbm, hbm, vmem, vmem, hbm],
            out_specs=(hbm, vmem, vmem, vmem, hbm),
            scratch_shapes=[
                pltpu.VMEM((units, 3, side, side, rows, hid), BF16),
                pltpu.VMEM((layers, tokens, d), BF16),
                pltpu.VMEM((layers, tokens, d), BF16),
                pltpu.VMEM((tokens, d), BF16),
                pltpu.VMEM((tokens, d), F32),
                pltpu.VMEM((2, 3, side, side, rows, hid), F32),
                pltpu.VMEM((2, 3, tile, hid), BF16),
                pltpu.VMEM((2, 2, tile, hid), F32),
                pltpu.VMEM((hid, hid), BF16),
                pltpu.VMEM((CHUNKS, 2, rows, hid), BF16),
                *[
                    pltpu.VMEM(shape, BF16)
                    for _ in range(2)
                    for shape in (
                        (2, 2, 3, side, rows, quarter),
                        (2, 2, 3, side, rows, half),
                        (2, 2, 3, rows, quarter),
                        (2, 2, 3, rows, half),
                    )
                ],
                pltpu.SemaphoreType.DMA((3,)),
                pltpu.SemaphoreType.DMA((2,)),
                pltpu.SemaphoreType.DMA((units, 4, 4)),
                pltpu.SemaphoreType.DMA((units, 4, 4)),
                pltpu.SemaphoreType.DMA((4, 4)),
                pltpu.SemaphoreType.DMA((4, 4)),
            ],
            compiler_params=pltpu.CompilerParams(
                collective_id=0, has_side_effects=True, vmem_limit_bytes=67_043_328
            ),
        )(x[0], dy[0], w_gate, w_up, w_down.reshape(units, rows, d))

        return by_x[None], by_gate, by_up, by_down.reshape(w_down.shape)

    tok, mat, grad = P(("rep", "dp")), P(None, "dp"), P("rep", "dp")
    return jax.shard_map(
        step,
        mesh=mesh,
        in_specs=(tok, tok, mat, mat, mat),
        out_specs=(tok, grad, grad, grad),
        check_vma=False,
    )
```

```python
import functools
import math

import jax
import jax.numpy as jnp
from jax import lax
from jax.experimental import pallas as pl
from jax.experimental.pallas import tpu as pltpu
from jax.sharding import PartitionSpec as P

F32, BF16 = jnp.float32, jnp.bfloat16
CHUNKS = 4
TILES = 8
EPS = 1e-6
HALVES = 2


def dot(a, b, ca, cb):
    return lax.dot_general(a, b, (((ca,), (cb,)), ((), ())), preferred_element_type=F32)


def kernel(
    side, layers, x_hbm, dy_hbm, gate_own, up_own, down_hbm, dx_hbm, out_gate, out_up, out_down, kept_hbm,
    w, h, a, dh, acc, g, s_tile, kept, order, fin, st1, st2, st3, st4, rc1, rc2, rc3, rc4,
    load_sem, keep_sem, ag_send, ag_recv, rs_send, rs_recv,
):
    tokens, d = h.shape[1:]
    rows, hid = w.shape[4:]
    tile = tokens // TILES
    half, quarter = hid // 2, hid // 4
    units = layers * CHUNKS
    me = lax.axis_index("dp")
    px, py = me // side, me % side
    xs = {k: (px + k + side) % side for k in (-1, 0, 1, 2)}
    ys = {k: (py + k + side) % side for k in (-1, 0, 1, 2)}
    beside = {
        ("x", 1): xs[1] * side + py,
        ("x", -1): xs[-1] * side + py,
        ("y", 1): px * side + ys[1],
        ("y", -1): px * side + ys[-1],
    }

    load_x = pltpu.make_async_copy(x_hbm, h.at[0], load_sem.at[0])
    load_dy = pltpu.make_async_copy(dy_hbm, dh, load_sem.at[1])
    load_w = pltpu.make_async_copy(down_hbm, w.at[:, 2, px, py], load_sem.at[2])
    load_w.start()
    load_x.start()
    load_dy.start()

    many = hid // (CHUNKS * rows)
    source = lax.broadcasted_iota(jnp.int32, (hid, hid), 0)
    goal = lax.broadcasted_iota(jnp.int32, (hid, hid), 1)
    chunk_of, place = goal // (many * rows), goal % (many * rows)
    at_source = (place // rows) * (CHUNKS * rows) + chunk_of * rows + place % rows
    order[...] = jnp.where(source == at_source, 1.0, 0.0).astype(BF16)
    run = many * rows
    owns = [(l, k, ref) for l in range(layers) for k, ref in enumerate((gate_own, up_own))]
    for q in range(CHUNKS):
        both = jnp.concatenate([ref[l, :, pl.ds(q * hid, hid)] for l, _, ref in owns], 0)
        moved = dot(both, order[...], 1, 0).astype(BF16)
        for n, (l, k, _) in enumerate(owns):
            for j in range(CHUNKS):
                piece = moved[n * rows : (n + 1) * rows, j * run : (j + 1) * run]
                w[l * CHUNKS + j, k, px, py, :, pl.ds(q * run, run)] = piece

    def finish(l):
        for q in range(CHUNKS):
            both = jnp.concatenate(
                [
                    jnp.concatenate([fin[j, k, :, pl.ds(q * run, run)] for j in range(CHUNKS)], 1)
                    for k in range(2)
                ],
                0,
            )
            moved = dot(both, order[...], 1, 1).astype(BF16)
            for k, ref in enumerate((out_gate, out_up)):
                ref[l, :, pl.ds(q * hid, hid)] = moved[k * rows : (k + 1) * rows]

    barrier = pltpu.get_barrier_semaphore()
    for target in beside.values():
        pl.semaphore_signal(barrier, inc=1, device_id={"dp": target})
    pl.semaphore_wait(barrier, len(beside))

    def gather_copies(u, s):
        copies = []
        for colour in range(2):
            axis = ("x", "y")[(colour + (s > 2)) % 2]
            for way, sign in ((0, 1), (1, -1)):
                lo = colour * half
                if s % 2:
                    lanes, at = pl.ds(lo, half), 0
                else:
                    lanes, at = pl.ds(lo + way * quarter, quarter), -sign
                pos = (xs if axis == "x" else ys)[at]
                if s <= 2:
                    i, j = (pos, py) if axis == "x" else (px, pos)
                else:
                    i, j = (pos, slice(None)) if axis == "x" else (slice(None), pos)
                ref = w.at[u, :, i, j, :, lanes]
                k = colour * 2 + way
                copies.append(
                    pltpu.make_async_remote_copy(
                        src_ref=ref,
                        dst_ref=ref,
                        send_sem=ag_send.at[u, s - 1, k],
                        recv_sem=ag_recv.at[u, s - 1, k],
                        device_id={"dp": beside[axis, sign]},
                    )
                )
        return copies

    def gather_done(u):
        for copy in gather_copies(u, 4):
            copy.wait()

    def gather_tick(k):
        for s in (4, 3, 2, 1):
            u = k - s + 1

            def step(s=s, u=u):
                if s > 1:
                    for copy in gather_copies(u, s - 1):
                        copy.wait()
                for copy in gather_copies(u, s):
                    copy.start()

            if isinstance(u, int):
                if 0 <= u < units:
                    step()
            else:
                pl.when(jnp.logical_and(u >= 0, u < units))(step)

    def reduce_copies(s):
        st, rc = ((st1, rc1), (st2, rc2), (st3, rc3), (st4, rc4))[s - 1]
        copies = []
        for colour in range(2):
            axis = ("x", "y")[(colour + (s > 2)) % 2]
            for way, sign in ((0, 1), (1, -1)):
                copies.append(
                    pltpu.make_async_remote_copy(
                        src_ref=st.at[colour, way],
                        dst_ref=rc.at[colour, way],
                        send_sem=rs_send.at[s - 1, colour * 2 + way],
                        recv_sem=rs_recv.at[s - 1, colour * 2 + way],
                        device_id={"dp": beside[axis, sign]},
                    )
                )
        return copies

    def part(par, colour, s, k, lo, n):
        axis = ("x", "y")[(colour + (s > 2)) % 2]
        pos = (xs if axis == "x" else ys)[k]
        lanes = pl.ds(colour * half + lo, n)
        if s <= 2:
            i, j = (pos, slice(None)) if axis == "x" else (slice(None), pos)
        else:
            i, j = (pos, py) if axis == "x" else (px, pos)
        return g.at[par, :, i, j, :, lanes]

    def begin(par, s):
        for colour in range(2):
            for way in range(2):
                (st1 if s == 1 else st3)[colour, way] = part(par, colour, s, 2, way * quarter, quarter)[...].astype(BF16)
        for copy in reduce_copies(s):
            copy.start()

    def middle(par, s):
        for copy in reduce_copies(s - 1):
            copy.wait()
        st, rc = (st2, rc1) if s == 2 else (st4, rc3)
        for colour in range(2):
            for way, sign in ((0, 1), (1, -1)):
                took, kept = way * quarter, (1 - way) * quarter
                st[colour, way, ..., pl.ds(took, quarter)] = (
                    part(par, colour, s, sign, took, quarter)[...] + rc[colour, way].astype(F32)
                ).astype(BF16)
                st[colour, way, ..., pl.ds(kept, quarter)] = part(par, colour, s, sign, kept, quarter)[...].astype(BF16)
        for copy in reduce_copies(s):
            copy.start()

    def reduce_tick(n, par, u):
        if n == 1:
            begin(par, 1)
        elif n == 2:
            middle(par, 2)
        elif n == 3:
            for copy in reduce_copies(2):
                copy.wait()
            for colour in range(2):
                own = part(par, colour, 2, 0, 0, half)
                own[...] = own[...] + rc2[colour, 0].astype(F32) + rc2[colour, 1].astype(F32)
            begin(par, 3)
        elif n == 4:
            middle(par, 4)
        else:
            for copy in reduce_copies(4):
                copy.wait()
            for colour in range(2):
                own = part(par, colour, 4, 0, 0, half)[...]
                total = own + rc4[colour, 0].astype(F32) + rc4[colour, 1].astype(F32)
                lanes = pl.ds(colour * half, half)
                fin[u % CHUNKS, :, :, lanes] = total[:2].astype(BF16)
                out_down[u, :, lanes] = total[2].astype(BF16)

    def at(t):
        return pl.ds(pl.multiple_of(t * tile, tile), tile)

    def matrix(u, k):
        return w[u, k].reshape(d, hid)

    def norm(l, t):
        wide = h[l, at(t)].astype(F32)
        scale = lax.rsqrt(jnp.mean(wide * wide, -1, keepdims=True) + EPS)
        a[l, at(t)] = (wide * scale).astype(BF16)

    def loop(n, body):
        lax.fori_loop(0, n, lambda i, c: (body(i), c)[1], 0)

    def keep(i):
        return pltpu.make_async_copy(kept.at[i % 2], kept_hbm.at[i], keep_sem.at[i % 2])

    def fetch(i):
        return pltpu.make_async_copy(kept_hbm.at[i], kept.at[i % 2], keep_sem.at[i % 2])

    def fwd1(i):
        u, t = i // TILES, i % TILES
        rowsa = a[0, at(t)]
        gate = dot(rowsa, matrix(u, 0), 1, 0)
        up = dot(rowsa, matrix(u, 1), 1, 0)
        kept[i % 2, 0] = gate
        kept[i % 2, 1] = up
        s_tile[i % 2, 2] = (gate * jax.nn.sigmoid(gate) * up).astype(BF16)

    def fwd2(i):
        u, t = i // TILES, i % TILES
        new = dot(s_tile[i % 2, 2], matrix(u, 2), 1, 0)
        acc[at(t)] = jnp.where(u == 0, 0.0, acc[at(t)]) + new

    def fwd_end(t):
        first = h[0, at(t)].astype(F32) + acc[at(t)].astype(BF16).astype(F32)
        h[1, at(t)] = first.astype(BF16)
        norm(1, t)

    def bwd1(l, i, late=False):
        u, t = l * CHUNKS + i // TILES, i % TILES
        n = tile // HALVES
        for r in range(HALVES):
            q = pl.ds(r * n, n)
            rr = pl.ds(pl.multiple_of(t * tile + r * n, n), n)
            if l:
                rowsa = a[l, rr]
                gate = dot(rowsa, matrix(u, 0), 1, 0)
                up = dot(rowsa, matrix(u, 1), 1, 0)
            else:
                gate, up = kept[i % 2, 0, q], kept[i % 2, 1, q]
            by = dot(dh[rr], matrix(u, 2), 1, 1).astype(BF16).astype(F32)
            sig = jax.nn.sigmoid(gate)
            silu = gate * sig
            by_gate = (by * up * (sig + silu * (1.0 - sig))).astype(BF16)
            by_up = (by * silu).astype(BF16)
            if late:
                h[1, rr] = by_gate
                a[1, rr] = by_up
            else:
                s_tile[i % 2, 0, q] = by_gate
                s_tile[i % 2, 1, q] = by_up
            s_tile[i % 2, 2, q] = (silu * up).astype(BF16)

    def by_hidden(i, late):
        t = i % TILES
        return (h[1, at(t)], a[1, at(t)]) if late else (s_tile[i % 2, 0], s_tile[i % 2, 1])

    def bwd_in(l, i, late=False):
        chunk, t = i // TILES, i % TILES
        u = l * CHUNKS + chunk
        by_gate, by_up = by_hidden(i, late)
        new = dot(by_gate, matrix(u, 0), 1, 1) + dot(by_up, matrix(u, 1), 1, 1)
        acc[at(t)] = jnp.where(chunk == 0, 0.0, acc[at(t)]) + new

    def bwd_w(l, i, late=False):
        chunk, t = i // TILES, i % TILES
        par = chunk % 2
        by_gate, by_up = by_hidden(i, late)
        rowsa = a[l, at(t)]
        for k, (p, q) in enumerate(((rowsa, by_gate), (rowsa, by_up), (s_tile[i % 2, 2], dh[at(t)]))):
            old = jnp.where(t == 0, 0.0, g[par, k])
            g[par, k] = old + dot(p, q, 0, 0).reshape(old.shape)

    def bwd_end(l, t):
        wide = h[l, at(t)].astype(F32)
        scale = lax.rsqrt(jnp.mean(wide * wide, -1, keepdims=True) + EPS)
        da = acc[at(t)].astype(BF16).astype(F32)
        along = jnp.mean(da * wide, -1, keepdims=True)
        by = (da * scale - wide * (scale * scale * scale * along)).astype(BF16)
        dh[at(t)] = (dh[at(t)].astype(F32) + by.astype(F32)).astype(BF16)

    load_w.wait()
    gather_tick(0)
    gather_tick(1)
    load_x.wait()
    loop(TILES // 2, lambda t: norm(0, t))
    gather_tick(2)
    loop(TILES - TILES // 2, lambda t: norm(0, t + TILES // 2))
    gather_tick(3)
    gather_done(0)

    steps = CHUNKS * TILES
    fwd1(0)
    keep(0).start()

    def fwd_step(i):
        @pl.when(i % TILES == 0)
        def _():
            gather_done(i // TILES)

        @pl.when(i % TILES == 2)
        def _():
            gather_tick(4 + i // TILES)

        @pl.when(i >= 2)
        def _():
            keep(i - 2).wait()

        fwd1(i)
        fwd2(i - 1)
        keep(i).start()

    loop(steps - 1, lambda i: fwd_step(i + 1))
    fwd2(steps - 1)
    loop(TILES, fwd_end)
    load_dy.wait()
    gather_done(CHUNKS)
    for i in (steps - 2, steps - 1):
        keep(i).wait()
    for i in range(2):
        fetch(i).start()

    when = ((1, 1), (2, 3), (3, 5), (4, 6), (5, 7))

    def step1(i):
        chunk, t = i // TILES, i % TILES

        @pl.when(t == 0)
        def _():
            gather_done(CHUNKS + chunk)

        @pl.when(t == 2)
        def _():
            gather_tick(4 + CHUNKS + chunk)

        for tick, place in when:

            @pl.when(jnp.logical_and(t == place, chunk > 0))
            def _(tick=tick):
                reduce_tick(tick, (chunk + 1) % 2, CHUNKS + chunk - 1)

        bwd_w(1, i - 1)
        bwd_in(1, i - 1)
        bwd1(1, i)

    bwd1(1, 0)
    loop(steps - 1, lambda i: step1(i + 1))
    bwd_in(1, steps - 1)
    bwd_w(1, steps - 1)
    loop(TILES, lambda t: bwd_end(1, t))

    def ticks(chunk, t):
        for tick, place in when:

            @pl.when(t == place)
            def _(tick=tick):
                reduce_tick(tick, (chunk + 1) % 2, (chunk + 2 * CHUNKS - 1) % (2 * CHUNKS))
                if tick == 5:
                    pl.when(chunk == 0)(lambda: finish(1))

    def step0(i):
        ticks(i // TILES, i % TILES)
        fetch(i + 1).start()
        fetch(i).wait()
        bwd_w(0, i - 1)
        bwd_in(0, i - 1)
        bwd1(0, i)

    def step0_late(i):
        ticks(i // TILES, i % TILES)
        pl.when(i + 1 < steps)(lambda: fetch(i + 1).start())
        fetch(i).wait()
        bwd1(0, i, True)
        bwd_w(0, i - 1, True)

    fetch(0).wait()
    bwd1(0, 0)
    early = steps - TILES
    loop(early - 1, lambda i: step0(i + 1))
    fetch(early + 1).start()
    fetch(early).wait()
    bwd1(0, early, True)
    bwd_in(0, early - 1)
    bwd_w(0, early - 1)
    loop(TILES - 1, lambda i: step0_late(i + early + 1))
    bwd_w(0, steps - 1, True)

    def end0(t):
        bwd_in(0, early + t, True)
        bwd_end(0, t)

    done = 0
    for tick, share in ((1, 2), (2, 3), (3, 1), (4, 2), (5, 0)):
        reduce_tick(tick, (CHUNKS - 1) % 2, CHUNKS - 1)
        if share:
            loop(share, lambda t, done=done: end0(t + done))
        done += share
        if tick == 4:
            store = pltpu.make_async_copy(dh, dx_hbm, load_sem.at[0])
            store.start()
    finish(0)
    store.wait()


def solution(mesh):
    ways = mesh.shape["dp"]
    side = math.isqrt(ways)

    def step(x, dy, w_gate, w_up, w_down):
        layers, rows, ff = w_gate.shape
        tokens, d = x.shape[1:]
        hid = ff // CHUNKS
        own = w_down.shape[1] // CHUNKS
        assert rows == own and d == hid and layers == 2
        units = layers * CHUNKS

        hbm, vmem = (pl.BlockSpec(memory_space=m) for m in (pl.ANY, pltpu.VMEM))
        tile = tokens // TILES
        quarter, half = hid // 4, hid // 2
        by_x, by_gate, by_up, by_down, _ = pl.pallas_call(
            functools.partial(kernel, side, layers),
            out_shape=(
                jax.ShapeDtypeStruct((tokens, d), BF16),
                jax.ShapeDtypeStruct(w_gate.shape, BF16),
                jax.ShapeDtypeStruct(w_up.shape, BF16),
                jax.ShapeDtypeStruct((units, rows, hid), BF16),
                jax.ShapeDtypeStruct((CHUNKS * TILES, 2, tile, hid), F32),
            ),
            in_specs=[hbm, hbm, vmem, vmem, hbm],
            out_specs=(hbm, vmem, vmem, vmem, hbm),
            scratch_shapes=[
                pltpu.VMEM((units, 3, side, side, rows, hid), BF16),
                pltpu.VMEM((layers, tokens, d), BF16),
                pltpu.VMEM((layers, tokens, d), BF16),
                pltpu.VMEM((tokens, d), BF16),
                pltpu.VMEM((tokens, d), F32),
                pltpu.VMEM((2, 3, side, side, rows, hid), F32),
                pltpu.VMEM((2, 3, tile, hid), BF16),
                pltpu.VMEM((2, 2, tile, hid), F32),
                pltpu.VMEM((hid, hid), BF16),
                pltpu.VMEM((CHUNKS, 2, rows, hid), BF16),
                *[
                    pltpu.VMEM(shape, BF16)
                    for _ in range(2)
                    for shape in (
                        (2, 2, 3, side, rows, quarter),
                        (2, 2, 3, side, rows, half),
                        (2, 2, 3, rows, quarter),
                        (2, 2, 3, rows, half),
                    )
                ],
                pltpu.SemaphoreType.DMA((3,)),
                pltpu.SemaphoreType.DMA((2,)),
                pltpu.SemaphoreType.DMA((units, 4, 4)),
                pltpu.SemaphoreType.DMA((units, 4, 4)),
                pltpu.SemaphoreType.DMA((4, 4)),
                pltpu.SemaphoreType.DMA((4, 4)),
            ],
            compiler_params=pltpu.CompilerParams(
                collective_id=0, has_side_effects=True, vmem_limit_bytes=67_043_328
            ),
        )(x[0], dy[0], w_gate, w_up, w_down.reshape(units, rows, d))

        return by_x[None], by_gate, by_up, by_down.reshape(w_down.shape)

    tok, mat, grad = P(("rep", "dp")), P(None, "dp"), P("rep", "dp")
    return jax.shard_map(
        step,
        mesh=mesh,
        in_specs=(tok, tok, mat, mat, mat),
        out_specs=(tok, grad, grad, grad),
        check_vma=False,
    )
```
